32 devices in a mesh: lat: 16 (over z, x, core), lev: 2 (over y).
Axes of the slice: x: 2, y: 2, z: 4, core: 2. Of those that a mesh axis runs over, the one named last changes fastest.
Arguments:
- anomalies: bfloat16 [4, 2, 80, 32, 1536], P(None, 'lev', None, 'lat'), may hold values from -6 to 6
- error_now: float32 [4, 2, 32, 1536], P(None, 'lev', 'lat'), may hold values from -6 to 6
- error_prior: float32 [4, 2, 32, 1536], P(None, 'lev', 'lat'), may hold values from -4.2 to 4.2
- energy_coef: float32 [4, 2], P(None, 'lev'), may hold values from 0.3 to 3
- obs_anomalies: bfloat16 [2048, 80, 256], P('lat', 'lev'), may hold values from -6 to 6
- innovations: float32 [2048, 256], P('lat'), may hold values from -6 to 6
- valid_counts: int32 [2048], P('lat'), may hold values from 0 to 256, as said below
- type_ids: int32 [2048], P('lat'), may hold values from 0 to 7
- error_inverse: float32 [8], replicated, may hold values from 0.25 to 4
Outputs:
- impact: float32 [2048, 16, 256], P('lat', 'lev')
- type_totals: float32 [16, 8], P('lev')
The draws below stay inside these ranges and needn't reach their ends.
Inputs may be any that keep to these rules, and one draw needn't show every extreme that they name: `valid_counts`: among the 128 slots of each index of lat, the blocks with a positive count come first and the first is always positive; in every draw some index of lat has all 128 slots positive and some block holds 256 rows. Rows below a block's count are observations, the rest padding.
All inputs are finite; a program needn't handle non-finite values.
Results may differ from the reference program's by a relative error of at most 0.0042.
Values may be sent and summed in bfloat16 or wider, within the bound.
No kernel may reach another device: no remote copies, remote signals or barrier semaphores. Data moves between devices by JAX's collectives and lax.ppermute only.
A program may use at most 64 MiB of HBM per device.

```python
import math
import jax
import jax.numpy as jnp
from jax import lax

K = 80
NLON = 1536
NLAT_GRID = 768
LAT0 = 256
VARS = 4
REGIONS = 4
BLOCK = 256
NTYPES = 8
SLOTS = 128
NLAT = 32
NLEV = 2
NBLK = 2048
N_LAT = 16


def draw_valid_counts(key, part):
    key_list = jax.random.split(key, 5)
    first_draw = jax.random.randint(key_list[0], (N_LAT,), 1, SLOTS + 1)
    second = jax.random.randint(key_list[1], (N_LAT,), 1, SLOTS + 1)
    device_loads = jnp.maximum(first_draw * second // SLOTS, 1)
    busiest = jax.random.randint(key_list[2], (), 0, N_LAT)
    device_index = jnp.arange(N_LAT, dtype=jnp.int32)
    device_loads = jnp.where(device_index == busiest, SLOTS, device_loads)
    slot_index = jnp.arange(SLOTS, dtype=jnp.int32)
    rows_drawn = jax.random.randint(key_list[3], (N_LAT, SLOTS), 3 * BLOCK // 4, BLOCK + 1)
    fullest = jax.random.randint(key_list[4], (), 0, SLOTS)
    chosen = (device_index[:, None] == busiest) & (slot_index[None, :] == fullest)
    rows_drawn = jnp.where(chosen, BLOCK, rows_drawn)
    counts = jnp.where(slot_index[None, :] < device_loads[:, None], rows_drawn, 0)
    return counts.reshape(N_LAT * SLOTS).astype(jnp.int32)


def with_ends(result, rng, least, top_value):
    longest = result.shape.index(max(result.shape))
    spots = []
    for shift in (0, 1):
        where = [jax.random.randint(jax.random.fold_in(rng, axis), (), 0, length) for axis, length in enumerate(result.shape)]
        where[longest] = (where[longest] + shift) % result.shape[longest]
        spots.append(tuple(where))
    return result.at[spots[0]].set(least).at[spots[1]].set(top_value)


def shard_levels(key, shape, cuts, least, top_value):
    def one(position, parts):
        steps = jax.random.uniform(jax.random.fold_in(jax.random.fold_in(key, 6), position), (parts,), jnp.float32, least / len(cuts), top_value / len(cuts))
        return jnp.repeat(jnp.exp(steps), shape[position] // parts).reshape((-1,) + (1,) * (len(shape) - position - 1))

    gain = one(*cuts[0])
    for cut in cuts[1:]:
        gain = gain * one(*cut)
    return gain


def normal_values(rng, extent, scale, bound, shards=(), held_as=jnp.bfloat16):
    gain = shard_levels(rng, extent, shards, -0.22, 0.18) if shards else 1.0
    result = jax.random.normal(rng, extent, jnp.float32) * scale * gain
    return jnp.minimum(jnp.maximum(result, -bound), bound).astype(held_as)


def setup_inputs(seed: int = 0) -> dict:
    seeds = jax.random.split(jax.random.key(seed), 10)
    anomalies = normal_values(seeds[0], (VARS, NLEV, K, NLAT, NLON), 1.0, 6.0, ((1, 2), (3, 16)))
    error_now = normal_values(seeds[1], (VARS, NLEV, NLAT, NLON), 1.0, 6.0, ((1, 2), (2, 16)), jnp.float32)
    error_prior = normal_values(seeds[2], (VARS, NLEV, NLAT, NLON), 0.7, 4.2, ((1, 2), (2, 16)), jnp.float32)
    energy_coef = jnp.clip(jnp.exp(math.log(3.0) - 2.3025851 * jax.random.uniform(seeds[3], (VARS, NLEV), jnp.float32) ** shard_levels(seeds[3], (VARS, NLEV), ((1, 2),), -0.2, 0.2)), 0.3, 3.0)
    obs_anomalies = normal_values(seeds[4], (NBLK, K, BLOCK), 1.0, 6.0, ((0, 16), (1, 2)))
    innovations = normal_values(seeds[5], (NBLK, BLOCK), 1.0, 6.0, ((0, 16),), jnp.float32)
    valid_counts = draw_valid_counts(jax.random.fold_in(seeds[9], 71), 0)
    type_ids = with_ends(jax.random.randint(seeds[7], (NBLK,), 0, NTYPES), jax.random.fold_in(seeds[7], 1), 0, NTYPES - 1).astype(jnp.int32)
    error_inverse = jnp.clip(jnp.exp(jax.random.uniform(seeds[8], (NTYPES,), jnp.float32, math.log(0.25), math.log(4.0))), 0.25, 4.0)
    return {"anomalies": anomalies, "error_now": error_now, "error_prior": error_prior, "energy_coef": energy_coef, "obs_anomalies": obs_anomalies, "innovations": innovations, "valid_counts": valid_counts, "type_ids": type_ids, "error_inverse": error_inverse}


def reference(anomalies, error_now, error_prior, energy_coef, obs_anomalies, innovations, valid_counts, type_ids, error_inverse):
    lat_index = jnp.arange(NLAT, dtype=jnp.int32)
    cosine = jnp.cos(-0.5 * math.pi + ((lat_index + LAT0).astype(jnp.float32) + 0.5) * math.pi / NLAT_GRID)
    gradient = (energy_coef[:, :, None, None] * cosine[None, None, :, None] * (error_now + error_prior)).astype(jnp.bfloat16)

    def level_sum(running, level_id):
        level_block = lax.dynamic_index_in_dim(anomalies, level_id, 1, keepdims=False)
        level_grad = lax.dynamic_index_in_dim(gradient, level_id, 1, keepdims=False)
        folded = jnp.einsum('vkji,vji->vkj', level_block.astype(jnp.float32), level_grad.astype(jnp.float32))
        return (running + folded, None)
    folded_all, _ = lax.scan(level_sum, jnp.zeros((VARS, K, NLAT), jnp.float32), jnp.arange(NLEV, dtype=jnp.int32))
    region = lat_index * REGIONS // NLAT
    onehot = (region[None, :] == jnp.arange(REGIONS, dtype=jnp.int32)[:, None]).astype(jnp.float32)
    member_sums = jnp.einsum('vkj,rj->vkr', folded_all, onehot, precision=lax.Precision.HIGHEST)
    norm_scale = math.sqrt(NLEV * NLAT * NLON / REGIONS)
    weights = (jnp.transpose(member_sums, (1, 0, 2)).reshape(K, VARS * REGIONS) / norm_scale).astype(jnp.bfloat16)
    response = jnp.einsum('bks,kt->bts', obs_anomalies.astype(jnp.float32), weights.astype(jnp.float32))
    type_table = type_ids[:, None] == jnp.arange(NTYPES, dtype=jnp.int32)[None, :]
    inverse_var = lax.optimization_barrier(jnp.sum(jnp.where(type_table, error_inverse[None, :], jnp.zeros((), jnp.float32)), axis=1))
    positions = jnp.arange(BLOCK, dtype=jnp.int32)
    row_mask = (positions[None, :] < valid_counts[:, None]).astype(jnp.float32)
    scaling = innovations * inverse_var[:, None] * row_mask / math.sqrt(K - 1)
    impact = response * scaling[:, None, :]
    per_block = lax.optimization_barrier(jnp.sum(impact, axis=2))
    type_totals = jnp.dot(per_block.T, type_table.astype(jnp.float32), precision=lax.Precision.HIGHEST) / math.sqrt(NBLK * BLOCK / NTYPES)
    return (impact, type_totals)
```

```python
import math

import jax
import jax.numpy as jnp
from jax import lax
from jax.sharding import PartitionSpec as P

NLAT_GRID = 768
LAT0 = 256
REGIONS = 4
NTYPES = 8


def exchange(value, axis, bit):
    size = lax.axis_size(axis)
    return lax.ppermute(value, axis, [(i, i ^ bit) for i in range(size)])


def butterfly(value, axis):
    bit = 1
    while bit < lax.axis_size(axis):
        value = value + exchange(value, axis, bit)
        bit *= 2
    return value


def local(
    anomalies,
    error_now,
    error_prior,
    energy_coef,
    obs_anomalies,
    innovations,
    valid_counts,
    type_ids,
    error_inverse,
):
    lat_rows = error_now.shape[2]
    lat_total = lat_rows * lax.axis_size("lat")
    lev_total = error_now.shape[1] * lax.axis_size("lev")
    lon_count = error_now.shape[3]
    variables = anomalies.shape[0]
    members = anomalies.shape[2]
    slot_count, local_members, block_rows = obs_anomalies.shape
    levs = lax.axis_size("lev")
    lev_index = lax.axis_index("lev")
    targets = variables * REGIONS
    own_targets = targets // levs

    lat_index = lax.axis_index("lat") * lat_rows + jnp.arange(lat_rows, dtype=jnp.int32)
    cosine = jnp.cos(
        -0.5 * math.pi + ((lat_index + LAT0).astype(jnp.float32) + 0.5) * math.pi / NLAT_GRID
    )
    gradient = (
        energy_coef[:, :, None, None] * cosine[None, None, :, None] * (error_now + error_prior)
    ).astype(jnp.bfloat16)
    folded = jnp.einsum("vlkji,vlji->vkj", anomalies, gradient, preferred_element_type=jnp.float32)
    region = lat_index * REGIONS // lat_total
    onehot = (region[None, :] == jnp.arange(REGIONS, dtype=jnp.int32)[:, None]).astype(jnp.float32)
    partial = jnp.einsum("vkj,rj->vrk", folded, onehot, precision=lax.Precision.HIGHEST)
    partial = butterfly(partial.reshape(targets, members), "lev")
    own = lax.dynamic_slice_in_dim(partial, lev_index * local_members, local_members, axis=1)

    type_table = type_ids[:, None] == jnp.arange(NTYPES, dtype=jnp.int32)[None, :]
    inverse_var = jnp.sum(
        jnp.where(type_table, error_inverse[None, :], jnp.zeros((), jnp.float32)), axis=1
    )
    positions = jnp.arange(block_rows, dtype=jnp.int32)
    row_mask = (positions[None, :] < valid_counts[:, None]).astype(jnp.float32)
    scaling = innovations * inverse_var[:, None] * row_mask / math.sqrt(members - 1)
    per_block = jnp.sum(obs_anomalies.astype(jnp.float32) * scaling[:, None, :], axis=2)
    per_type = jnp.einsum(
        "bc,bk->ck", type_table.astype(jnp.float32), per_block, precision=lax.Precision.HIGHEST
    )

    summed = butterfly(jnp.concatenate([own, per_type], axis=0), "lat")
    norm_scale = math.sqrt(lev_total * lat_total * lon_count / REGIONS)
    weights = (summed[:targets] / norm_scale).astype(jnp.bfloat16)
    per_type = summed[targets:]

    weight_parts = weights.reshape(levs, own_targets, local_members)
    total_parts = jnp.einsum(
        "tk,ck->tc", weights.astype(jnp.float32), per_type, precision=lax.Precision.HIGHEST
    ).reshape(levs, own_targets, NTYPES)

    def respond(part):
        return jnp.einsum(
            "bks,tk->bts", obs_anomalies, part, preferred_element_type=jnp.float32
        )

    def pick(parts, index):
        return lax.dynamic_index_in_dim(parts, index, 0, keepdims=False)

    received = []
    total_received = []
    for step in range(1, levs):
        perm = [(i, (i + step) % levs) for i in range(levs)]
        peer = (lev_index + step) % levs
        sent = respond(pick(weight_parts, peer)).astype(jnp.bfloat16)
        received.append(lax.ppermute(sent, "lev", perm))
        total_received.append(lax.ppermute(pick(total_parts, peer), "lev", perm))
    response = respond(pick(weight_parts, lev_index))
    for part in received:
        response = response + part.astype(jnp.float32)
    impact = response * scaling[:, None, :]
    totals = pick(total_parts, lev_index)
    for part in total_received:
        totals = totals + part
    block_total = slot_count * lax.axis_size("lat")
    type_totals = totals / math.sqrt(block_total * block_rows / NTYPES)
    return (impact, type_totals)


def solution(mesh):
    in_specs = (
        P(None, "lev", None, "lat", None),
        P(None, "lev", "lat", None),
        P(None, "lev", "lat", None),
        P(None, "lev"),
        P("lat", "lev", None),
        P("lat", None),
        P("lat"),
        P("lat"),
        P(),
    )
    out_specs = (P("lat", "lev", None), P("lev", None))
    return jax.shard_map(local, mesh=mesh, in_specs=in_specs, out_specs=out_specs, check_vma=False)
```

```python
import math

import jax
import jax.numpy as jnp
from jax import lax
from jax.sharding import PartitionSpec as P


NLAT_GRID = 768
LAT0 = 256
REGIONS = 4
NTYPES = 8
STEPS = 4


def exchange(value, axis, bit):
    size = lax.axis_size(axis)
    return lax.ppermute(value, axis, [(i, i ^ bit) for i in range(size)])


def butterfly(value, axis):
    bit = 1
    while bit < lax.axis_size(axis):
        value = value + exchange(value, axis, bit)
        bit *= 2
    return value


def turned(value, axis, index):
    levs = lax.axis_size("lev")
    unit = value.shape[axis] // levs
    result = value
    for part in range(1, levs):
        head = lax.slice_in_dim(value, part * unit, value.shape[axis], axis=axis)
        tail = lax.slice_in_dim(value, 0, part * unit, axis=axis)
        result = jnp.where(index == part, jnp.concatenate([head, tail], axis=axis), result)
    return result


def local(
    anomalies,
    error_now,
    error_prior,
    energy_coef,
    obs_anomalies,
    innovations,
    valid_counts,
    type_ids,
    error_inverse,
):
    lat_rows = error_now.shape[2]
    lat_total = lat_rows * lax.axis_size("lat")
    lev_total = error_now.shape[1] * lax.axis_size("lev")
    lon_count = error_now.shape[3]
    variables = anomalies.shape[0]
    members = anomalies.shape[2]
    slot_count, local_members, block_rows = obs_anomalies.shape
    levs = lax.axis_size("lev")
    lev_index = lax.axis_index("lev")
    targets = variables * REGIONS
    own_targets = targets // levs
    shifts = [[(i, (i + step) % levs) for i in range(levs)] for step in range(levs)]

    lev_index, first_lat, error_now = lax.optimization_barrier(
        (lev_index, lax.axis_index("lat") * lat_rows, error_now)
    )

    lat_index = first_lat + jnp.arange(lat_rows, dtype=jnp.int32)
    cosine = jnp.cos(
        -0.5 * math.pi + ((lat_index + LAT0).astype(jnp.float32) + 0.5) * math.pi / NLAT_GRID
    )
    gradient = (
        (error_now + error_prior) * cosine[None, None, :, None] * energy_coef[:, :, None, None]
    ).astype(jnp.bfloat16)
    folded = jnp.einsum("vlkji,vlji->vkj", anomalies, gradient, preferred_element_type=jnp.float32)
    region = lat_index * REGIONS // lat_total
    onehot = (region[None, :] == jnp.arange(REGIONS, dtype=jnp.int32)[:, None]).astype(jnp.float32)
    partial = jnp.einsum("vkj,rj->vrk", folded, onehot, precision=lax.Precision.HIGHEST)
    partial = partial.reshape(targets, members)
    partial = butterfly(partial, "lev")
    partial = turned(turned(partial, 0, lev_index), 1, lev_index)

    type_table = type_ids[:, None] == jnp.arange(NTYPES, dtype=jnp.int32)[None, :]
    inverse_var = jnp.sum(
        jnp.where(type_table, error_inverse[None, :], jnp.zeros((), jnp.float32)), axis=1
    )
    positions = jnp.arange(block_rows, dtype=jnp.int32)
    row_mask = (positions[None, :] < valid_counts[:, None]).astype(jnp.float32)
    scaling = innovations * inverse_var[:, None] * row_mask / math.sqrt(members - 1)
    per_block = jnp.sum(obs_anomalies.astype(jnp.float32) * scaling[:, None, :], axis=2)
    per_type = jnp.einsum(
        "bc,bk->ck", type_table.astype(jnp.float32), per_block, precision=lax.Precision.HIGHEST
    )
    per_type = jnp.pad(per_type, ((0, 0), (0, members - local_members)))

    unit = slot_count // STEPS
    summed = jnp.concatenate([partial, per_type], axis=0)
    length = None
    bit = 1
    while bit < lax.axis_size("lat"):
        if bit == 2:
            summed, valid_counts = lax.optimization_barrier((summed, valid_counts))
        if bit == 4:
            summed, near_obs = lax.optimization_barrier((summed, obs_anomalies))
            near_obs = jnp.maximum(near_obs, jnp.finfo(near_obs.dtype).min)
            near_obs = lax.optimization_barrier(near_obs)
        added = exchange(summed, "lat", bit)
        if bit == 2:
            place = jnp.arange(slot_count, dtype=jnp.int32)
            marks = (valid_counts > 0) & (place > 0) & (place % unit == 0)
            length = jnp.sum(marks.astype(jnp.int32))
            summed, added, length = lax.optimization_barrier((summed, added, length))
        summed = summed + added
        bit *= 2
    norm_scale = math.sqrt(lev_total * lat_total * lon_count / REGIONS)
    weights = (summed[:targets] / norm_scale).astype(jnp.bfloat16)
    per_type = summed[targets:, :local_members]

    def respond(obs, part):
        return jnp.einsum("bks,tk->bts", obs, part, preferred_element_type=jnp.float32)

    def total_of(part):
        return jnp.einsum(
            "tk,ck->tc", part.astype(jnp.float32), per_type, precision=lax.Precision.HIGHEST
        )

    far = range(1, levs)
    parts = [
        weights[step * own_targets : (step + 1) * own_targets, :local_members]
        for step in range(levs)
    ]
    totals = [total_of(part) for part in parts]

    def finish(blocks):
        def run(obs, scaling, parts, totals):
            sent = [
                lax.optimization_barrier(respond(obs[:blocks], parts[step]).astype(jnp.bfloat16))
                for step in far
            ]
            received = []
            total = totals[0]
            for step in far:
                total = total + lax.ppermute(totals[step], "lev", shifts[step])
                received.append(lax.ppermute(sent[step - 1], "lev", shifts[step]))
            response = lax.optimization_barrier(respond(obs[:blocks], parts[0]))
            for part in received:
                response = response + part.astype(jnp.float32)
            impact = response * scaling[:blocks, None, :]
            block_total = slot_count * lax.axis_size("lat")
            total = total / math.sqrt(block_total * block_rows / NTYPES)
            return jnp.pad(impact, ((0, slot_count - blocks), (0, 0), (0, 0))), total

        return run

    return lax.switch(
        length,
        [finish((i + 1) * unit) for i in range(STEPS)],
        near_obs,
        scaling,
        parts,
        totals,
    )


def solution(mesh):
    in_specs = (
        P(None, "lev", None, "lat", None),
        P(None, "lev", "lat", None),
        P(None, "lev", "lat", None),
        P(None, "lev"),
        P("lat", "lev", None),
        P("lat", None),
        P("lat"),
        P("lat"),
        P(),
    )
    out_specs = (P("lat", "lev", None), P("lev", None))

    return jax.shard_map(local, mesh=mesh, in_specs=in_specs, out_specs=out_specs, check_vma=False)
```

```python
import math

import jax
import jax.numpy as jnp
from jax import lax
from jax.sharding import PartitionSpec as P


NLAT_GRID = 768
LAT0 = 256
REGIONS = 4
NTYPES = 8
EARLY = (7, 32)
STEPS = 10


def exchange(value, axis, bit):
    size = lax.axis_size(axis)
    return lax.ppermute(value, axis, [(i, i ^ bit) for i in range(size)])


def butterfly(value, axis):
    bit = 1
    while bit < lax.axis_size(axis):
        value = value + exchange(value, axis, bit)
        bit *= 2
    return value


def turned(value, axis, index):
    levs = lax.axis_size("lev")
    unit = value.shape[axis] // levs
    result = value
    for part in range(1, levs):
        head = lax.slice_in_dim(value, part * unit, value.shape[axis], axis=axis)
        tail = lax.slice_in_dim(value, 0, part * unit, axis=axis)
        result = jnp.where(index == part, jnp.concatenate([head, tail], axis=axis), result)
    return result


def local(
    anomalies,
    error_now,
    error_prior,
    energy_coef,
    obs_anomalies,
    innovations,
    valid_counts,
    type_ids,
    error_inverse,
):
    lat_rows = error_now.shape[2]
    lat_total = lat_rows * lax.axis_size("lat")
    lev_total = error_now.shape[1] * lax.axis_size("lev")
    lon_count = error_now.shape[3]
    variables = anomalies.shape[0]
    members = anomalies.shape[2]
    slot_count, local_members, block_rows = obs_anomalies.shape
    levs = lax.axis_size("lev")
    lev_index = lax.axis_index("lev")
    targets = variables * REGIONS
    own_targets = targets // levs
    shifts = [[(i, (i + step) % levs) for i in range(levs)] for step in range(levs)]

    lev_index, first_lat, error_now = lax.optimization_barrier(
        (lev_index, lax.axis_index("lat") * lat_rows, error_now)
    )

    lat_index = first_lat + jnp.arange(lat_rows, dtype=jnp.int32)
    cosine = jnp.cos(
        -0.5 * math.pi + ((lat_index + LAT0).astype(jnp.float32) + 0.5) * math.pi / NLAT_GRID
    )
    gradient = (
        (error_now + error_prior) * cosine[None, None, :, None] * energy_coef[:, :, None, None]
    ).astype(jnp.bfloat16)
    folded = jnp.einsum("vlkji,vlji->vkj", anomalies, gradient, preferred_element_type=jnp.float32)
    region = lat_index * REGIONS // lat_total
    onehot = (region[None, :] == jnp.arange(REGIONS, dtype=jnp.int32)[:, None]).astype(jnp.float32)
    partial = jnp.einsum("vkj,rj->vrk", folded, onehot, precision=lax.Precision.HIGHEST)
    partial = partial.reshape(targets, members)
    partial = butterfly(partial, "lev")
    partial = turned(turned(partial, 0, lev_index), 1, lev_index)

    unit = (slot_count - slot_count * EARLY[0] // EARLY[1]) // STEPS
    early = slot_count - STEPS * unit
    first_obs = lax.optimization_barrier(obs_anomalies[:early])
    early_obs = []
    for step in range(1, levs):
        early_obs.append(lax.ppermute(first_obs, "lev", shifts[step]))

    type_table = type_ids[:, None] == jnp.arange(NTYPES, dtype=jnp.int32)[None, :]
    inverse_var = jnp.sum(
        jnp.where(type_table, error_inverse[None, :], jnp.zeros((), jnp.float32)), axis=1
    )
    positions = jnp.arange(block_rows, dtype=jnp.int32)
    row_mask = (positions[None, :] < valid_counts[:, None]).astype(jnp.float32)
    scaling = innovations * inverse_var[:, None] * row_mask / math.sqrt(members - 1)
    per_block = jnp.sum(obs_anomalies.astype(jnp.float32) * scaling[:, None, :], axis=2)
    per_type = jnp.einsum(
        "bc,bk->ck", type_table.astype(jnp.float32), per_block, precision=lax.Precision.HIGHEST
    )
    per_type = jnp.pad(per_type, ((0, 0), (0, members - local_members)))

    place = jnp.arange(slot_count, dtype=jnp.int32)
    marks = (valid_counts > 0) & (place >= early) & ((place - early) % unit == 0)
    length = jnp.sum(marks.astype(jnp.int32))
    summed = jnp.concatenate([partial, per_type], axis=0)
    bit = 1
    while bit < lax.axis_size("lat"):
        if bit == 4:
            summed, near_obs = lax.optimization_barrier((summed, obs_anomalies))
            near_obs = jnp.maximum(near_obs, jnp.finfo(near_obs.dtype).min)
            near_obs = lax.optimization_barrier(near_obs)
        if bit in (1,) and 4 * bit <= lax.axis_size("lat"):
            added = [exchange(summed, "lat", bit * i) for i in (1, 2, 3)]
            summed = (summed + added[0]) + (added[1] + added[2])
            bit *= 4
        else:
            summed = summed + exchange(summed, "lat", bit)
            bit *= 2
    norm_scale = math.sqrt(lev_total * lat_total * lon_count / REGIONS)
    weights = (summed[:targets] / norm_scale).astype(jnp.bfloat16)
    per_type = summed[targets:, :local_members]

    def respond(obs, part):
        return jnp.einsum("bks,tk->bts", obs, part, preferred_element_type=jnp.float32)

    def total_of(part):
        return jnp.einsum(
            "tk,ck->tc", part.astype(jnp.float32), per_type, precision=lax.Precision.HIGHEST
        )

    far = range(1, levs)
    parts = [
        weights[step * own_targets : (step + 1) * own_targets, :local_members]
        for step in range(levs)
    ]
    totals = [total_of(part) for part in parts]

    early_parts = []
    for step in far:
        low = (levs - step) * local_members
        early_parts.append(weights[:own_targets, low : low + local_members])

    def finish(late):
        blocks = early + late

        def run(obs, early_obs, scaling, parts, early_parts, totals):
            total = totals[0]
            received = []
            for step in far:
                moved = lax.ppermute(totals[step], "lev", shifts[step])
                total = total + moved
                if late:
                    pieces = []
                    for low, high in ((early, blocks - unit), (blocks - unit, blocks)):
                        if low < high:
                            sent = respond(obs[low:high], parts[step]).astype(jnp.bfloat16)
                            sent = lax.optimization_barrier(sent)
                            pieces.append(lax.ppermute(sent, "lev", shifts[step]))
                    received.append(jnp.concatenate(pieces, axis=0))
            own = lax.optimization_barrier(respond(obs[:blocks], parts[0]))
            first = own[:early]
            for step in far:
                first = first + respond(early_obs[step - 1], early_parts[step - 1])
            response = lax.optimization_barrier(first)
            if late:
                rest = own[early:]
                for part in received:
                    rest = rest + part.astype(jnp.float32)
                response = jnp.concatenate([response, rest], axis=0)
            impact = response * scaling[:blocks, None, :]
            block_total = slot_count * lax.axis_size("lat")
            total = total / math.sqrt(block_total * block_rows / NTYPES)
            return jnp.pad(impact, ((0, slot_count - blocks), (0, 0), (0, 0))), total

        return run

    return lax.switch(
        length,
        [finish(i * unit) for i in range(STEPS + 1)],
        near_obs,
        early_obs,
        scaling,
        parts,
        early_parts,
        totals,
    )


def solution(mesh):
    in_specs = (
        P(None, "lev", None, "lat", None),
        P(None, "lev", "lat", None),
        P(None, "lev", "lat", None),
        P(None, "lev"),
        P("lat", "lev", None),
        P("lat", None),
        P("lat"),
        P("lat"),
        P(),
    )
    out_specs = (P("lat", "lev", None), P("lev", None))

    return jax.shard_map(local, mesh=mesh, in_specs=in_specs, out_specs=out_specs, check_vma=False)
```

```python
import math

import jax
import jax.numpy as jnp
from jax import lax
from jax.sharding import PartitionSpec as P


NLAT_GRID = 768
LAT0 = 256
REGIONS = 4
NTYPES = 8
EARLY = (4, 32)
STEPS = 16


def exchange(value, axis, bit):
    size = lax.axis_size(axis)
    return lax.ppermute(value, axis, [(i, i ^ bit) for i in range(size)])


def butterfly(value, axis):
    bit = 1
    while bit < lax.axis_size(axis):
        value = value + exchange(value, axis, bit)
        bit *= 2
    return value


def turned(value, axis, index):
    levs = lax.axis_size("lev")
    unit = value.shape[axis] // levs
    result = value
    for part in range(1, levs):
        head = lax.slice_in_dim(value, part * unit, value.shape[axis], axis=axis)
        tail = lax.slice_in_dim(value, 0, part * unit, axis=axis)
        result = jnp.where(index == part, jnp.concatenate([head, tail], axis=axis), result)
    return result


def local(
    anomalies,
    error_now,
    error_prior,
    energy_coef,
    obs_anomalies,
    innovations,
    valid_counts,
    type_ids,
    error_inverse,
):
    lat_rows = error_now.shape[2]
    lat_total = lat_rows * lax.axis_size("lat")
    lev_total = error_now.shape[1] * lax.axis_size("lev")
    lon_count = error_now.shape[3]
    variables = anomalies.shape[0]
    members = anomalies.shape[2]
    slot_count, local_members, block_rows = obs_anomalies.shape
    levs = lax.axis_size("lev")
    lev_index = lax.axis_index("lev")
    targets = variables * REGIONS
    own_targets = targets // levs
    shifts = [[(i, (i + step) % levs) for i in range(levs)] for step in range(levs)]

    lev_index, first_lat, error_now = lax.optimization_barrier(
        (lev_index, lax.axis_index("lat") * lat_rows, error_now)
    )

    lat_index = first_lat + jnp.arange(lat_rows, dtype=jnp.int32)
    cosine = jnp.cos(
        -0.5 * math.pi + ((lat_index + LAT0).astype(jnp.float32) + 0.5) * math.pi / NLAT_GRID
    )
    gradient = (
        (error_now + error_prior) * cosine[None, None, :, None] * energy_coef[:, :, None, None]
    ).astype(jnp.bfloat16)
    lat_index = first_lat + jnp.arange(lat_rows, dtype=jnp.int32)
    region = lat_index * REGIONS // lat_total
    if lat_total % (REGIONS * lat_rows) == 0:
        folded = jnp.einsum(
            "vlkji,vlji->vk", anomalies, gradient, preferred_element_type=jnp.float32
        )
        mine = region[0] == jnp.arange(REGIONS, dtype=jnp.int32)
        partial = jnp.where(mine[None, :, None], folded[:, None, :], jnp.zeros((), jnp.float32))
    else:
        folded = jnp.einsum(
            "vlkji,vlji->vkj", anomalies, gradient, preferred_element_type=jnp.float32
        )
        onehot = region[None, :] == jnp.arange(REGIONS, dtype=jnp.int32)[:, None]
        partial = jnp.einsum(
            "vkj,rj->vrk", folded, onehot.astype(jnp.float32), precision=lax.Precision.HIGHEST
        )
    partial = partial.reshape(targets, members)
    partial = butterfly(partial, "lev")
    partial = turned(turned(partial, 0, lev_index), 1, lev_index)

    unit = (slot_count - slot_count * EARLY[0] // EARLY[1]) // STEPS
    early = slot_count - STEPS * unit
    first_obs = lax.optimization_barrier(obs_anomalies[:early])
    early_obs = []
    for step in range(1, levs):
        early_obs.append(lax.ppermute(first_obs, "lev", shifts[step]))

    type_table = type_ids[:, None] == jnp.arange(NTYPES, dtype=jnp.int32)[None, :]
    positions = jnp.arange(block_rows, dtype=jnp.int32)
    row_mask = (positions[None, :] < valid_counts[:, None]).astype(jnp.float32)
    root = math.sqrt(members - 1)
    per_block = jnp.sum(
        obs_anomalies.astype(jnp.float32) * (innovations * row_mask)[:, None, :], axis=2
    )
    per_type = jnp.einsum(
        "bc,bk->ck", type_table.astype(jnp.float32), per_block, precision=lax.Precision.HIGHEST
    )
    per_type = per_type * error_inverse[:, None] / root

    per_type, late_innovations, late_counts, late_types = lax.optimization_barrier(
        (per_type, innovations, valid_counts, type_ids)
    )
    late_table = late_types[:, None] == jnp.arange(NTYPES, dtype=jnp.int32)[None, :]
    inverse_var = jnp.sum(
        jnp.where(late_table, error_inverse[None, :], jnp.zeros((), jnp.float32)), axis=1
    )
    inverse_var = lax.optimization_barrier(inverse_var)
    late_mask = (positions[None, :] < late_counts[:, None]).astype(jnp.float32)
    scaling = late_innovations * inverse_var[:, None] * late_mask / root
    scaling = lax.optimization_barrier(scaling)
    per_type = jnp.pad(per_type, ((0, 0), (0, members - local_members)))

    place = jnp.arange(slot_count, dtype=jnp.int32)
    marks = (valid_counts > 0) & (place >= early) & ((place - early) % unit == 0)
    length = jnp.sum(marks.astype(jnp.int32))
    summed = jnp.concatenate([partial, per_type], axis=0)
    bit = 1
    while bit < lax.axis_size("lat"):
        if bit == 4:
            summed, near_obs = lax.optimization_barrier((summed, obs_anomalies))
            near_obs = jnp.maximum(near_obs, jnp.finfo(near_obs.dtype).min)
            near_obs = lax.optimization_barrier(near_obs)
        if bit in (1,) and 4 * bit <= lax.axis_size("lat"):
            added = [exchange(summed, "lat", bit * i) for i in (1, 2, 3)]
            summed = (summed + added[0]) + (added[1] + added[2])
            bit *= 4
        else:
            summed = summed + exchange(summed, "lat", bit)
            bit *= 2
    norm_scale = math.sqrt(lev_total * lat_total * lon_count / REGIONS)
    weights = (summed[:targets] / norm_scale).astype(jnp.bfloat16)
    per_type = summed[targets:, :local_members]

    def respond(obs, part):
        return jnp.einsum("bks,tk->bts", obs, part, preferred_element_type=jnp.float32)

    def total_of(part, per_type):
        return jnp.einsum(
            "tk,ck->tc", part.astype(jnp.float32), per_type, precision=lax.Precision.HIGHEST
        )

    far = range(1, levs)
    parts = [
        weights[step * own_targets : (step + 1) * own_targets, :local_members]
        for step in range(levs)
    ]

    early_parts = []
    for step in far:
        low = (levs - step) * local_members
        early_parts.append(weights[:own_targets, low : low + local_members])

    def finish(late):
        blocks = early + late
        middle = early + late // unit // 2 * unit

        def run(obs, early_obs, scaling, parts, early_parts, per_type):
            totals = [lax.optimization_barrier(total_of(part, per_type)) for part in parts]
            total = totals[0]
            received = []
            for step in far:
                moved = lax.ppermute(totals[step], "lev", shifts[step])
                total = total + moved
                if late:
                    pieces = []
                    for low, high in ((early, middle), (middle, blocks)):
                        if low < high:
                            sent = respond(obs[low:high], parts[step]).astype(jnp.bfloat16)
                            sent = lax.optimization_barrier(sent)
                            pieces.append(lax.ppermute(sent, "lev", shifts[step]))
                    received.append(pieces)
            own = lax.optimization_barrier(respond(obs[:blocks], parts[0]))
            first = own[:early]
            for step in far:
                first = first + respond(early_obs[step - 1], early_parts[step - 1])
            response = lax.optimization_barrier(first)

            def scaled(response, low, high):
                return response * scaling[low:high, None, :]

            def arrived(piece, low, high):
                rest = own[low:high]
                for part in received:
                    rest = rest + part[piece].astype(jnp.float32)
                return rest

            if middle > early:
                response = jnp.concatenate([response, arrived(0, early, middle)], axis=0)
            impact = jnp.pad(
                scaled(response, 0, middle), ((0, slot_count - middle), (0, 0), (0, 0))
            )
            if late:
                impact = lax.optimization_barrier(impact)
                rest = scaled(arrived(-1, middle, blocks), middle, blocks)
                impact = lax.dynamic_update_slice(impact, rest, (middle, 0, 0))
            block_total = slot_count * lax.axis_size("lat")
            total = total / math.sqrt(block_total * block_rows / NTYPES)
            return impact, total

        return run

    return lax.switch(
        length,
        [finish(i * unit) for i in range(STEPS + 1)],
        near_obs,
        early_obs,
        scaling,
        parts,
        early_parts,
        per_type,
    )


def solution(mesh):
    in_specs = (
        P(None, "lev", None, "lat", None),
        P(None, "lev", "lat", None),
        P(None, "lev", "lat", None),
        P(None, "lev"),
        P("lat", "lev", None),
        P("lat", None),
        P("lat"),
        P("lat"),
        P(),
    )
    out_specs = (P("lat", "lev", None), P("lev", None))

    return jax.shard_map(local, mesh=mesh, in_specs=in_specs, out_specs=out_specs, check_vma=False)
```
